32 devices in a mesh: seq: 16 (over z, y, x), fsdp: 2 (over core).
Axes of the slice: x: 2, y: 2, z: 4, core: 2. Of those that a mesh axis runs over, the one named last changes fastest.
Arguments:
- tokens: bfloat16 [2, 12288, 2560], P('fsdp', 'seq'), may hold values from -6 to 6
- bounds: int32 [2, 16, 2], P('fsdp', 'seq'), may hold values from 0 to 24, as said below
- in_weight: bfloat16 [2560, 5416], P(('seq', 'fsdp')), may hold values from -0.125 to 0.125
- conv_weight: float32 [4, 2816], replicated, may hold values from -0.6 to 0.6
- conv_bias: float32 [2816], replicated, may hold values from -3 to 3
- dt_bias: float32 [40], replicated, may hold values from -4 to 0
- decay_rate: float32 [40], replicated, may hold values from 4.8828125e-05 to 0.5
- skip_gain: float32 [40], replicated, may hold values from 0.1 to 1.9
- norm_gain: float32 [2560], replicated, may hold values from 0.1 to 1.9
Outputs:
- layer_out: bfloat16 [2, 12288, 2560], P('fsdp', 'seq')
The draws below stay inside these ranges and needn't reach their ends.
Inputs may be any that keep to these rules, and one draw needn't show every extreme that they name: For sequence b, bounds[b, s] holds the first and one past the last block of the shard of index s of seq; shards are consecutive in s and cover all 24 blocks; each holds 1 to 3 blocks, and some shard holds 3.
All inputs are finite; a program needn't handle non-finite values.
Results may differ from the reference program's by a relative error of at most 0.0028.
The reference program's roundings to bfloat16 on the way count: a program that leaves them out, or rounds other values in their place, can miss the bound.
Values may be sent and summed in bfloat16 or wider, within the bound.
No kernel may reach another device: no remote copies, remote signals or barrier semaphores. Data moves between devices by JAX's collectives and lax.ppermute only.
A program may use at most 192 MiB of HBM per device.

```python
import jax
import jax.numpy as jnp
from jax import lax

D = 2560
HEADS = 40
HEAD_DIM = 64
STATE = 128
CONV = 4
BLOCK = 256
SLOT_BLOCKS = 3
INNER = 2560
COLS = 5416
SLOTS = 768
TOTAL_BLOCKS = 24
SEQ_LEN = 6144
SEQS = 2
N_SEQ = 16


def draw_bounds(key, part):
    rows = []
    for index in range(SEQS):
        subkey = jax.random.fold_in(key, 11 + index)
        pick_key, order_key = jax.random.split(subkey)
        heavy = jax.random.randint(pick_key, (), 1, N_SEQ // 4 + 1)
        middle = N_SEQ // 2 - 2 * heavy
        ranking = jax.random.permutation(order_key, N_SEQ)
        counts = jnp.where(ranking < heavy, 3, jnp.where(ranking < heavy + middle, 2, 1)).astype(jnp.int32)
        ends = jnp.cumsum(counts).astype(jnp.int32)
        rows.append(jnp.stack([ends - counts, ends], axis=1))
    return jnp.stack(rows).astype(jnp.int32)


def draw_decay_rate(key, part):
    choose_key, value_key = jax.random.split(jax.random.fold_in(key, 5))
    slow_heads = jax.random.uniform(choose_key, (HEADS,)) < 0.5
    spread = jax.random.uniform(value_key, (HEADS,), jnp.float32)
    slow_rate = 0.3 / SEQ_LEN * jnp.exp(spread * jnp.log(10.0))
    fast_rate = 0.05 * jnp.exp(spread * jnp.log(10.0))
    return jnp.where(slow_heads, slow_rate, fast_rate).astype(jnp.float32)


def levels(rng, shape, shards, low, largest):
    gain = 1.0
    for position, shards_of in shards:
        draws = jax.random.uniform(jax.random.fold_in(jax.random.fold_in(rng, 6), position), (shards_of,), jnp.float32, low / len(shards), largest / len(shards))
        gain = gain * jnp.repeat(jnp.exp(draws), shape[position] // shards_of).reshape((-1,) + (1,) * (len(shape) - 1 - position))
    return gain


def noise(stream_key, shape, scale, limit, cuts=(), dtype=jnp.bfloat16):
    array = scale * jax.random.normal(stream_key, shape, jnp.float32)
    if cuts:
        array = array * levels(stream_key, shape, cuts, -0.22, 0.18)
    return jnp.clip(array, -limit, limit).astype(dtype)


def setup_inputs(seed: int = 0) -> dict:
    arg_keys = jax.random.split(jax.random.key(seed), 10)
    tokens = noise(arg_keys[0], (SEQS, N_SEQ * SLOTS, D), 1.0, 6.0, ((0, 2), (1, 16)))
    bounds = draw_bounds(jax.random.fold_in(arg_keys[9], 71), 0)
    in_weight = noise(arg_keys[2], (D, COLS), D ** -0.5, 0.125, ((0, 32),))
    conv_weight = jnp.clip(jax.random.uniform(arg_keys[3], (CONV, INNER + 2 * STATE), jnp.float32, -0.6, 0.6), -0.6, 0.6)
    conv_bias = noise(arg_keys[4], (INNER + 2 * STATE,), 0.5, 3.0, (), jnp.float32)
    dt_bias = jnp.clip(jax.random.uniform(arg_keys[5], (HEADS,), jnp.float32, -4.0, 0.0), -4.0, 0.0)
    decay_rate = draw_decay_rate(jax.random.fold_in(arg_keys[9], 71), 0)
    skip_gain = jnp.clip(1.0 + 0.18 * jax.random.normal(arg_keys[7], (HEADS,), jnp.float32), 0.1, 1.9)
    norm_gain = jnp.clip(1.0 + 0.18 * jax.random.normal(arg_keys[8], (INNER,), jnp.float32), 0.1, 1.9)
    return dict(tokens=tokens, bounds=bounds, in_weight=in_weight, conv_weight=conv_weight, conv_bias=conv_bias, dt_bias=dt_bias, decay_rate=decay_rate, skip_gain=skip_gain, norm_gain=norm_gain)


def block_terms(head_input, input_map, output_map, step_size, decay_rate):
    log_decay = -(step_size * decay_rate[None, :]).T
    cumulative = jnp.cumsum(log_decay, axis=1)
    pairwise = cumulative[:, :, None] - cumulative[:, None, :]
    length = cumulative.shape[1]
    causal = jnp.arange(length)[:, None] >= jnp.arange(length)[None, :]
    pair_decay = jnp.exp(jnp.where(causal[None], pairwise, -jnp.inf))
    scores = jnp.dot(output_map, input_map.T, preferred_element_type=jnp.float32)
    mixing = scores[None] * pair_decay * step_size.T[:, None, :]
    inner_out = jnp.einsum('hij,jhp->ihp', mixing, head_input, precision=lax.Precision.HIGH)
    to_end = jnp.exp(cumulative[:, -1:] - cumulative) * step_size.T
    local_state = jnp.einsum('hj,jhp,jn->hpn', to_end, head_input, input_map.astype(jnp.float32), precision=lax.Precision.HIGH)
    return (inner_out, cumulative, local_state)

def carried(output_map, cumulative, state):
    reach = jnp.einsum('in,hpn->ihp', output_map.astype(jnp.float32), state, precision=lax.Precision.HIGH)
    return jnp.exp(cumulative).T[:, :, None] * reach

def one_sequence(tokens, bounds, in_weight, conv_weight, conv_bias, dt_bias, decay_rate, skip_gain, norm_gain):
    starts = bounds[:, 0]
    ends = bounds[:, 1]
    blocks = jnp.arange(TOTAL_BLOCKS).astype(jnp.int32)
    owner = lax.optimization_barrier(jnp.sum((ends[None, :] <= blocks[:, None]).astype(jnp.int32), axis=1)).astype(jnp.int32)
    slot_row = (owner * SLOT_BLOCKS + blocks - starts[owner]).astype(jnp.int32)
    grouped = tokens.reshape(N_SEQ * SLOT_BLOCKS, BLOCK, D)
    live = grouped[slot_row].reshape(SEQ_LEN, D)
    projected = jnp.dot(live, in_weight, preferred_element_type=jnp.float32).astype(jnp.bfloat16)
    gate = projected[:, :INNER].astype(jnp.float32)
    mixed_in = projected[:, INNER:2 * INNER + 2 * STATE]
    raw_step = projected[:, 2 * INNER + 2 * STATE:].astype(jnp.float32)
    padded = jnp.concatenate([jnp.zeros((CONV - 1, mixed_in.shape[1]), jnp.bfloat16), mixed_in], axis=0)
    convolved = jnp.zeros((SEQ_LEN, mixed_in.shape[1]), jnp.float32) + conv_bias[None, :]
    for offset in range(CONV):
        convolved = convolved + conv_weight[offset][None, :] * padded[offset:offset + SEQ_LEN].astype(jnp.float32)
    conv_out = jax.nn.silu(convolved).astype(jnp.bfloat16)
    head_input = conv_out[:, :INNER].astype(jnp.float32).reshape(TOTAL_BLOCKS, BLOCK, HEADS, HEAD_DIM)
    input_map = conv_out[:, INNER:INNER + STATE].reshape(TOTAL_BLOCKS, BLOCK, STATE)
    output_map = conv_out[:, INNER + STATE:].reshape(TOTAL_BLOCKS, BLOCK, STATE)
    step_size = jax.nn.softplus(raw_step + dt_bias[None, :]).reshape(TOTAL_BLOCKS, BLOCK, HEADS)

    def advance(state, pieces):
        in_values, in_map, out_map, in_step = pieces
        inner_out, cumulative, local_state = block_terms(in_values, in_map, out_map, in_step, decay_rate)
        result = inner_out + carried(out_map, cumulative, state) + skip_gain[None, :, None] * in_values
        state = jnp.exp(cumulative[:, -1])[:, None, None] * state + local_state
        return (state, result)
    initial = jnp.zeros((HEADS, HEAD_DIM, STATE), jnp.float32)
    final_state, outputs = lax.scan(advance, initial, (head_input, input_map, output_map, step_size))
    scanned = outputs.reshape(SEQ_LEN, INNER)
    gated = scanned * jax.nn.silu(gate)
    normed = gated * lax.rsqrt(lax.optimization_barrier(jnp.mean(gated * gated, axis=1, keepdims=True)) + 1e-05) * norm_gain[None, :]
    placed = jnp.zeros((N_SEQ * SLOT_BLOCKS, BLOCK, INNER), jnp.bfloat16)
    placed = placed.at[slot_row].set(normed.astype(jnp.bfloat16).reshape(TOTAL_BLOCKS, BLOCK, INNER))
    return placed.reshape(N_SEQ * SLOTS, INNER)

def reference(tokens, bounds, in_weight, conv_weight, conv_bias, dt_bias, decay_rate, skip_gain, norm_gain):
    results = [one_sequence(tokens[index], bounds[index], in_weight, conv_weight, conv_bias, dt_bias, decay_rate, skip_gain, norm_gain) for index in range(SEQS)]
    return jnp.stack(results)
```

```python
import functools

import jax
import jax.numpy as jnp
import numpy as np
from jax import lax
from jax.experimental import pallas as pl
from jax.experimental.pallas import tpu as pltpu
from jax.sharding import PartitionSpec as P


BLOCK = 256
TILE = 256
LANES = 128
HALO = 16
AXES = ("seq", "fsdp")
LOG2E = 1.4426950408889634
VMEM = pltpu.VMEM
F32 = jnp.float32
BF16 = jnp.bfloat16


def split2(f):
    hi = f.astype(BF16)
    return hi, (f - hi.astype(F32)).astype(BF16)


def split3(f):
    hi = f.astype(BF16)
    rest = f - hi.astype(F32)
    mid = rest.astype(BF16)
    return hi, mid, (rest - mid.astype(F32)).astype(BF16)


def dot(a, b):
    return jnp.dot(a, b, preferred_element_type=F32)


def dot_rows(a, b):
    return lax.dot_general(a, b, (((0,), (0,)), ((), ())), preferred_element_type=F32)


def packed(f, heads):
    lane = lax.broadcasted_iota(jnp.int32, f.shape, 1)
    keep = lambda v: jnp.where(lane < heads, v, 0.0)
    hi = f.astype(BF16).astype(F32)
    mid = (f - hi).astype(BF16).astype(F32)
    lo = f - hi - mid
    return (keep(hi) + pltpu.roll(keep(mid), heads, 1) + pltpu.roll(keep(lo), 2 * heads, 1)).astype(BF16)


def expander(width, first_head, head_dim, heads):
    row = lax.broadcasted_iota(jnp.int32, (LANES, width), 0)
    lane = lax.broadcasted_iota(jnp.int32, (LANES, width), 1)
    head = row - jnp.where(row >= 2 * heads, 2 * heads, jnp.where(row >= heads, heads, 0))
    low = (head - first_head) * head_dim
    return jnp.where((lane >= low) & (lane < low + head_dim) & (row < 3 * heads), 1.0, 0.0).astype(BF16)


def silu(a):
    return a * (1.0 / (1.0 + jnp.exp(-a)))


def weight_copies(pieces, offsets_ref, weight, sem, rows, low, high):
    copies = []
    number = 0
    for piece in pieces:
        for part in range(piece.shape[0] // rows):
            to = pl.multiple_of(offsets_ref[number], 16)
            at = pl.ds(low, high - low)
            copies.append(
                pltpu.make_async_copy(
                    piece.at[pl.ds(part * rows, rows), at], weight.at[pl.ds(to, rows), at], sem
                )
            )
            number += 1
    return copies


def begin(copies):
    for copy in copies:
        copy.start()


def finish(copies):
    for copy in copies:
        copy.wait()


def project_kernel(count, rows, base, extra, has_step, *refs):
    offsets_ref, blocks_ref = refs[:2]
    pieces = refs[2 : 2 + count]
    refs = refs[2 + count :]
    if has_step:
        tokens, halo, taps, bias, scalars = refs[:5]
        out, step_out, cum_out, ext, weight, acc, sem = refs[5:]
    else:
        tokens, halo, taps, bias = refs[:4]
        out, ext, weight, acc, sem = refs[4:]
    slots = tokens.shape[0]
    width = weight.shape[1]
    tiles = out.shape[1] // TILE
    plain = tiles - (1 if has_step else 0)
    first_tiles = 2
    cut = first_tiles * TILE
    inputs = [
        pltpu.make_async_copy(halo, ext.at[pl.ds(0, HALO), :], sem.at[0]),
        pltpu.make_async_copy(tokens, ext.at[pl.ds(HALO, slots), :], sem.at[0]),
    ]
    inputs += weight_copies(pieces, offsets_ref, weight, sem.at[0], rows, 0, cut)
    others = weight_copies(pieces, offsets_ref, weight, sem.at[1], rows, cut, width)
    begin(inputs)
    begin(others)
    finish(inputs)
    kernel = taps.shape[0]

    def epilogue(t, slot):
        column = jnp.where(t < plain, base + t * TILE, extra)
        from_ = pl.ds(pl.multiple_of(column, LANES), TILE)
        at = pl.ds(pl.multiple_of(t * TILE, TILE), TILE)
        tap = taps[:, from_]
        start = bias[:, from_]
        for block in range(slots // BLOCK):
            total = start + jnp.zeros((BLOCK, TILE), F32)
            for k in range(kernel):
                first = HALO - (kernel - 1) + k + block * BLOCK
                total = total + tap[k : k + 1, :] * acc[slot, first : first + BLOCK, :]
            out[block * BLOCK : (block + 1) * BLOCK, at] = silu(total).astype(BF16)

    def tile(t, carry):
        epilogue(jnp.maximum(t - 1, 0), lax.rem(t + 1, 2))
        at = pl.ds(pl.multiple_of(t * TILE, TILE), TILE)
        acc[lax.rem(t, 2)] = dot(ext[...], weight[:, at]).astype(BF16).astype(F32)
        return carry

    lax.fori_loop(0, first_tiles, tile, 0)
    finish(others)
    lax.fori_loop(first_tiles, tiles, tile, 0)
    if has_step:
        first = tiles * TILE
        raw_all = dot(ext[HALO:, :], weight[:, first : first + LANES]).astype(BF16).astype(F32)
        row = lax.broadcasted_iota(jnp.int32, (BLOCK, BLOCK), 0)
        col = lax.broadcasted_iota(jnp.int32, (BLOCK, BLOCK), 1)
        lower = jnp.where(row >= col, 1.0, 0.0).astype(BF16)
        token = lax.broadcasted_iota(jnp.int32, (BLOCK, LANES), 0)
        for block in range(slots // BLOCK):
            low, high = block * BLOCK, (block + 1) * BLOCK
            a = raw_all[low:high] + scalars[0:1, :]
            size = jnp.maximum(a, 0.0) + jnp.log1p(jnp.exp(-jnp.abs(a)))
            size = jnp.where(token + low < blocks_ref[0] * BLOCK, size, 0.0)
            hi, mid, lo = split3(-(size * scalars[1:2, :]))
            step_out[low:high, :] = size
            cum_out[low:high, :] = dot(lower, hi) + dot(lower, mid) + dot(lower, lo)
    epilogue(tiles - 1, (tiles - 1) % 2)


def summary_kernel(first_head, head_dim, heads, x_ref, bc_ref, cum_ref, step_ref, starts, summary, state, total):
    width = x_ref.shape[1]
    state_width = bc_ref.shape[1] // 2
    block = pl.program_id(0)

    @pl.when(block == 0)
    def _():
        state[...] = jnp.zeros_like(state)
        total[...] = jnp.ones_like(total)

    onehot = expander(width, first_head, head_dim, heads)
    cum = cum_ref[...]
    last = cum[BLOCK - 1 : BLOCK, :]
    to_end = dot(packed(jnp.exp(last - cum) * step_ref[...], heads), onehot)
    hi, lo = split2(x_ref[...].astype(F32) * to_end)
    b = bc_ref[:, :state_width]
    local = dot_rows(b, hi) + dot_rows(b, lo)
    decay = dot(packed(jnp.exp(last) + jnp.zeros((8, LANES), F32), heads), onehot)
    starts[0] = state[...]
    state[...] = decay[:1, :] * state[...] + local
    total[...] = total[...] * decay

    @pl.when(block == pl.num_programs(0) - 1)
    def _():
        quarter = summary.shape[2]
        for q in range(summary.shape[0]):
            summary[q, :state_width, :] = state[:, q * quarter : (q + 1) * quarter]
            summary[q, state_width:, :] = total[:, q * quarter : (q + 1) * quarter]


def inner_kernel(first_head, head_dim, heads, x_ref, bc_ref, cum_ref, step_ref, scalars, starts, y_ref):
    width = x_ref.shape[1]
    state_width = bc_ref.shape[1] // 2
    half = BLOCK // 2
    b = bc_ref[:, :state_width]
    c = bc_ref[:, state_width:]
    scores = lax.dot_general(c, b, (((1,), (1,)), ((), ())), preferred_element_type=F32)
    cum = cum_ref[...]
    step = step_ref[...]
    scaled = cum * LOG2E
    log_step = jnp.where(step > 0.0, jnp.log(step) * LOG2E, -1e30)
    across = (log_step - scaled).T
    onehot = expander(width, first_head, head_dim, heads)
    reach_decay = dot(packed(jnp.exp(cum), heads), onehot)
    skip = dot(packed(scalars[2:3, :] + jnp.zeros((8, LANES), F32), heads), onehot)
    row = lax.broadcasted_iota(jnp.int32, (half, half), 0)
    col = lax.broadcasted_iota(jnp.int32, (half, half), 1)
    causal = row >= col
    lane = lax.broadcasted_iota(jnp.int32, (1, LANES), 1)
    per = LANES // head_dim
    cc = jnp.concatenate([c, c], axis=1)
    for group in range(width // LANES):
        at = slice(group * LANES, (group + 1) * LANES)
        x = x_ref[:, at]
        reach = dot(cc, jnp.concatenate(split2(starts[0, :, at]), axis=0))
        base = reach * reach_decay[:, at] + skip[:1, at] * x.astype(F32)
        top, low = base[:half], base[half:]
        for member in range(per):
            head = first_head + group * per + member
            mine = (lane >= member * head_dim) & (lane < (member + 1) * head_dim)
            own = jnp.where(mine, x, jnp.zeros_like(x))
            down = scaled[:, head : head + 1]
            right = across[head : head + 1, :]
            m00 = jnp.where(causal, jnp.exp2(down[:half] + right[:, :half]) * scores[:half, :half], 0.0)
            m10 = jnp.exp2(down[half:] + right[:, :half]) * scores[half:, :half]
            m11 = jnp.where(causal, jnp.exp2(down[half:] + right[:, half:]) * scores[half:, half:], 0.0)
            hi, lo = split2(m00)
            top = top + (dot(hi, own[:half]) + dot(lo, own[:half]))
            hi, lo = split2(jnp.concatenate([m10, m11], axis=1))
            low = low + (dot(hi, own) + dot(lo, own))
        y_ref[:half, at] = top
        y_ref[half:, at] = low


def gate_kernel(count, rows, *refs):
    offsets_ref = refs[0]
    pieces = refs[1 : 1 + count]
    tokens_hbm, out, tokens, weight, sem = refs[1 + count :]
    width = weight.shape[1]
    inputs = [pltpu.make_async_copy(tokens_hbm, tokens, sem.at[0])]
    inputs += weight_copies(pieces, offsets_ref, weight, sem.at[0], rows, 0, TILE)
    others = weight_copies(pieces, offsets_ref, weight, sem.at[1], rows, TILE, width)
    begin(inputs)
    begin(others)
    finish(inputs)

    def tile(t, carry):
        at = pl.ds(pl.multiple_of(t * TILE, TILE), TILE)
        out[:, at] = dot(tokens[...], weight[:, at]).astype(BF16)
        return carry

    tile(0, 0)
    finish(others)
    lax.fori_loop(1, width // TILE, tile, 0)


def final_kernel(head_dim, heads, blocks_ref, *refs):
    gates, ys, states = refs[:2], refs[2:4], refs[4:6]
    bc_ref, cum_ref, gain, out, earlier, gated = refs[6:]
    state_width = bc_ref.shape[1] // 2
    whole = out.shape[1]
    block = pl.program_id(0)

    @pl.when(block == 0)
    def _():
        earlier[...] = jnp.zeros_like(earlier)

    def part(pair, column):
        first = pair[0].shape[1]
        ref, low = (pair[0], column) if column < first else (pair[1], column - first)
        return ref[:, low : low + TILE]

    cum = cum_ref[...]
    factors = packed(jnp.exp(cum + earlier[:1, :]), heads)
    earlier[...] = earlier[...] + cum[BLOCK - 1 : BLOCK, :]
    c = bc_ref[:, state_width:]
    twice = jnp.concatenate([c, c], axis=1)
    squares = jnp.zeros((BLOCK, LANES), F32)
    for column in range(0, whole, TILE):
        both = jnp.concatenate(split2(part(states, column)), axis=0)
        reach = dot(twice, both)
        decay = dot(factors, expander(TILE, column // head_dim, head_dim, heads))
        value = (part(ys, column) + decay * reach) * silu(part(gates, column).astype(F32))
        gated[:, column : column + TILE] = value
        square = value * value
        for lane in range(0, TILE, LANES):
            squares = squares + square[:, lane : lane + LANES]
    scale = lax.rsqrt(jnp.sum(squares, axis=1, keepdims=True) / whole + 1e-05)
    live = block < blocks_ref[0]
    for column in range(0, whole, TILE):
        at = slice(column, column + TILE)
        out[:, at] = jnp.where(live, gated[:, at] * scale * gain[:, at], 0.0).astype(BF16)


HBM = pl.BlockSpec(memory_space=pltpu.HBM)
FULL = pl.BlockSpec(memory_space=pltpu.VMEM)
SCALARS = pl.BlockSpec(memory_space=pltpu.SMEM)
MIB = 1024 * 1024


def like(shape, dtype):
    return jax.ShapeDtypeStruct(shape, dtype)


def call(kernel, in_specs, out_shape, scratch, flops, limit, *args):
    return pl.pallas_call(
        kernel,
        in_specs=in_specs,
        out_specs=jax.tree.map(lambda _: FULL, out_shape),
        out_shape=out_shape,
        scratch_shapes=scratch,
        cost_estimate=pl.CostEstimate(flops=flops, bytes_accessed=16_000_000, transcendentals=0),
        compiler_params=pltpu.CompilerParams(vmem_limit_bytes=limit * MIB),
    )(*args)


def project(pieces, rows, offsets, blocks, tokens, halo, taps, bias, base, extra, scalars):
    slots, depth = tokens.shape
    width = pieces[0].shape[1]
    has_step = scalars is not None
    conv = width - LANES if has_step else width
    out = [like((slots, conv), BF16)]
    if has_step:
        out += [like((slots, LANES), F32)] * 2
    return call(
        functools.partial(project_kernel, len(pieces), rows, base, extra, has_step),
        [SCALARS] * 2 + [HBM] * (len(pieces) + 2) + [FULL] * (3 if has_step else 2),
        out,
        [
            VMEM((slots + HALO, depth), BF16),
            VMEM((depth, width), BF16),
            VMEM((2, slots + HALO, TILE), F32),
            pltpu.SemaphoreType.DMA((2,)),
        ],
        2 * slots * depth * width, 40,
        offsets, blocks, *pieces, tokens, halo, taps, bias, *([scalars] if has_step else []),
    )


def by_block(width, column=0):
    return pl.BlockSpec((BLOCK, width), lambda i: (i, column))


def summarize(x, width, first, bc_at, state_width, cum, step, first_head, head_dim, heads, parts):
    slots = x.shape[0]
    count = slots // BLOCK
    shape = (parts, state_width + 8, width // parts)
    return pl.pallas_call(
        functools.partial(summary_kernel, first_head, head_dim, heads),
        name="summary",
        grid=(count,),
        in_specs=[by_block(width), by_block(2 * state_width, bc_at), by_block(LANES), by_block(LANES)],
        out_specs=[
            pl.BlockSpec((1, state_width, width), lambda i: (i, 0, 0)),
            pl.BlockSpec(shape, lambda i: (0, 0, 0)),
        ],
        out_shape=[like((count, state_width, width), F32), like(shape, F32)],
        scratch_shapes=[VMEM((state_width, width), F32), VMEM((8, width), F32)],
        cost_estimate=pl.CostEstimate(flops=4 * slots * state_width * width, bytes_accessed=8_000_000, transcendentals=0),
        compiler_params=pltpu.CompilerParams(vmem_limit_bytes=40 * MIB),
    )(x, first, cum, step)


def inner(x, width, first, bc_at, state_width, cum, step, scalars, starts, first_head, head_dim, heads):
    slots = x.shape[0]
    return pl.pallas_call(
        functools.partial(inner_kernel, first_head, head_dim, heads),
        name="inner",
        grid=(slots // BLOCK,),
        in_specs=[
            by_block(width), by_block(2 * state_width, bc_at), by_block(LANES), by_block(LANES),
            pl.BlockSpec((8, LANES), lambda i: (0, 0)),
            pl.BlockSpec((1, state_width, width), lambda i: (i, 0, 0)),
        ],
        out_specs=by_block(width),
        out_shape=like((slots, width), F32),
        cost_estimate=pl.CostEstimate(flops=6 * slots * BLOCK * width, bytes_accessed=8_000_000, transcendentals=0),
        compiler_params=pltpu.CompilerParams(vmem_limit_bytes=40 * MIB),
    )(x, first, cum, step, scalars, starts)


def gate_columns(pieces, rows, offsets, tokens):
    slots, depth = tokens.shape
    width = pieces[0].shape[1]
    return call(
        functools.partial(gate_kernel, len(pieces), rows),
        [SCALARS] + [HBM] * (len(pieces) + 1),
        like((slots, width), BF16),
        [VMEM((slots, depth), BF16), VMEM((depth, width), BF16), pltpu.SemaphoreType.DMA((2,))],
        2 * slots * depth * width, 32,
        offsets, *pieces, tokens,
    )


def finished(blocks, gates, ys, states, first, bc_at, state_width, cum, gain, head_dim, heads):
    slots = cum.shape[0]
    whole = gain.shape[1]
    full = lambda a: pl.BlockSpec(a.shape, lambda i: (0, 0))
    return pl.pallas_call(
        functools.partial(final_kernel, head_dim, heads),
        name="final",
        grid=(slots // BLOCK,),
        in_specs=[SCALARS] + [by_block(a.shape[1]) for a in gates + ys] + [full(a) for a in states]
        + [by_block(2 * state_width, bc_at), by_block(LANES), full(gain)],
        out_specs=by_block(whole),
        out_shape=like((slots, whole), BF16),
        scratch_shapes=[VMEM((8, LANES), F32), VMEM((BLOCK, whole), F32)],
        cost_estimate=pl.CostEstimate(flops=8 * slots * state_width * whole, bytes_accessed=16_000_000, transcendentals=0),
        compiler_params=pltpu.CompilerParams(vmem_limit_bytes=40 * MIB),
    )(blocks, *gates, *ys, *states, first, cum, gain)


PLANE = 4


def routes(planes, cores):
    ids = lambda z, m, c: (z * PLANE + m) * cores + c
    places = [(z, m, c) for z in range(planes) for m in range(PLANE) for c in range(cores)]
    beside = lambda turn: [(ids(z, m, c), ids(z, m ^ (1 if c % 2 == turn else 2), c)) for z, m, c in places]
    return dict(
        long=[[(ids(z, m, c), ids((z + k) % planes, m, c)) for z, m, c in places] for k in range(planes)],
        beside=[beside(0), beside(1)],
        swap=[(ids(z, m, c), ids(z, m, cores - 1 - c)) for z, m, c in places],
        cross=[[(ids(z, m, c), ids(z, m ^ a, c)) for z, m, c in places] for a in range(PLANE)],
        later=[[(ids(z, m, c), ids(z + k, m, c)) for z, m, c in places if z + k < planes] for k in range(planes)],
        after=[(s, s + cores) for s in range((planes * PLANE - 1) * cores)],
    )


def send(value, pairs):
    return lax.ppermute(value, AXES, pairs)


def moved(held, pairs):
    value, blocks = held
    landed = np.zeros_like(blocks)
    for source, target in pairs:
        landed[target] = blocks[source]
    return send(value, pairs), landed


def joined(parts):
    return jnp.concatenate([v for v, _ in parts], axis=0), np.concatenate([b for _, b in parts], axis=1)


def along(held, paths, planes):
    return [held] + [moved(held, paths["long"][k]) for k in range(1, planes)]


def around(held, paths):
    near = moved(held, paths["beside"][0])
    side = moved(held, paths["beside"][1])
    return [held, near, side, moved(near, paths["beside"][1])]


def collect(chunk, paths, planes, cores, rows, place, long_first):
    if rows % HALO or planes > PLANE:
        return [lax.all_gather(chunk, AXES, axis=0, tiled=True)], jnp.zeros((1,), jnp.int32), rows * planes * PLANE * cores
    own = (chunk, np.arange(planes * PLANE * cores)[:, None])
    if long_first:
        line = around(joined(along(own, paths, planes)), paths)
    else:
        line = along(joined(around(own, paths)), paths, planes)
    line = line + [moved(held, paths["swap"]) for held in line]
    table = np.concatenate([b for _, b in line], axis=1) * rows
    return [v for v, _ in line], jnp.asarray(table, jnp.int32)[place], rows


def compose(earlier, later, wide):
    decay = later[wide:]
    return jnp.concatenate([decay[:1] * earlier[:wide] + later[:wide], earlier[wide:] * decay], axis=0)


def pick(parts, index):
    return lax.dynamic_index_in_dim(parts, index, 0, False)


def carried_in(summary, paths, planes, mine, wide):
    parts = jnp.stack(
        [pick(summary, mine)]
        + [send(pick(summary, mine ^ a), paths["cross"][a]) for a in range(1, PLANE)]
    )
    members = [pick(parts, mine ^ m) for m in range(PLANE)]
    totals = [members[0]]
    for member in members[1:]:
        totals.append(compose(totals[-1], member, wide))
    state = jnp.zeros_like(summary[0, :wide])
    for k in range(planes - 1, 0, -1):
        part = send(totals[-1], paths["later"][k])
        state = part[wide : wide + 1] * state + part[:wide]
    states = jnp.stack([state] + [t[wide : wide + 1] * state + t[:wide] for t in totals[:-1]])
    back = jnp.stack([pick(states, mine)] + [send(pick(states, mine ^ a), paths["cross"][a]) for a in range(1, PLANE)])
    return jnp.concatenate([pick(back, mine ^ q) for q in range(PLANE)], axis=1)


def local(tokens, bounds, in_weight, conv_weight, conv_bias, dt_bias, decay_rate, skip_gain, norm_gain):
    cores = lax.axis_size("fsdp")
    planes = lax.axis_size("seq") // PLANE
    place = lax.axis_index("seq") * cores + lax.axis_index("fsdp")
    mine = lax.axis_index("seq") % PLANE
    paths = routes(planes, cores)
    own = tokens[0]
    rows = in_weight.shape[0]
    inner_width = norm_gain.shape[0]
    state_width = (conv_bias.shape[0] - inner_width) // 2
    heads = decay_rate.shape[0]
    head_dim = inner_width // heads
    early = heads * 2 // 5 // 8 * 8
    cut = early * head_dim
    live = bounds[0, 0, 1] - bounds[0, 0, 0]
    blocks = live[None]
    scalars = jnp.pad(jnp.stack([dt_bias, decay_rate, skip_gain]), ((0, 5), (0, LANES - heads)))

    rest = jnp.pad(in_weight[:, 2 * inner_width :], ((0, 0), (0, LANES - heads)))
    chunks = [
        jnp.concatenate([in_weight[:, inner_width : inner_width + cut], rest], axis=1),
        in_weight[:, inner_width + cut : 2 * inner_width],
        in_weight[:, : inner_width - cut],
        in_weight[:, inner_width - cut : inner_width],
    ]
    edge = lax.dynamic_slice_in_dim(own, live * BLOCK - HALO, HALO, 0)
    halo = send(edge, paths["after"])
    weights = [collect(chunk, paths, planes, cores, rows, place, i < LONG_FIRST) for i, chunk in enumerate(chunks)]

    bias = conv_bias[None]
    first, step, cum = project(
        weights[0][0], weights[0][2], weights[0][1], blocks, own, halo, conv_weight, bias, 0, inner_width, scalars
    )
    (second,) = project(
        weights[1][0], weights[1][2], weights[1][1], blocks, own, halo, conv_weight, bias, cut, cut, None
    )
    x = [first, second]
    widths = [cut, inner_width - cut]
    firsts = [0, early]
    bc_at = cut // (2 * state_width)
    parts, states, ys = [], [], []
    for i in range(2):
        parts.append(
            summarize(x[i], widths[i], first, bc_at, state_width, cum, step, firsts[i], head_dim, heads, PLANE)
        )
    for i in range(2):
        states.append(carried_in(parts[i][1], paths, planes, mine, state_width))
    for i in range(2):
        ys.append(
            inner(x[i], widths[i], first, bc_at, state_width, cum, step, scalars, parts[i][0], firsts[i], head_dim, heads)
        )
    gates = []
    for i in range(2):
        gates.append(gate_columns(weights[2 + i][0], weights[2 + i][2], weights[2 + i][1], own))
    out = finished(blocks, gates, ys, states, first, bc_at, state_width, cum, norm_gain[None], head_dim, heads)
    return out[None]


LONG_FIRST = 3


def solution(mesh):
    whole = P("fsdp", "seq", None)
    in_specs = (whole, whole, P(("seq", "fsdp"), None)) + (P(),) * 6

    return jax.shard_map(local, mesh=mesh, in_specs=in_specs, out_specs=whole, check_vma=False)
```

```python
import functools

import jax
import jax.numpy as jnp
import numpy as np
from jax import lax
from jax.experimental import pallas as pl
from jax.experimental.pallas import tpu as pltpu
from jax.sharding import PartitionSpec as P


BLOCK = 256
TILE = 256
LANES = 128
HALO = 16
AXES = ("seq", "fsdp")
LOG2E = 1.4426950408889634
VMEM = pltpu.VMEM
F32 = jnp.float32
BF16 = jnp.bfloat16


def split2(f):
    hi = f.astype(BF16)
    return hi, (f - hi.astype(F32)).astype(BF16)


def split3(f):
    hi = f.astype(BF16)
    rest = f - hi.astype(F32)
    mid = rest.astype(BF16)
    return hi, mid, (rest - mid.astype(F32)).astype(BF16)


def dot(a, b):
    return jnp.dot(a, b, preferred_element_type=F32)


def dot_rows(a, b):
    return lax.dot_general(a, b, (((0,), (0,)), ((), ())), preferred_element_type=F32)


def packed(f, heads):
    lane = lax.broadcasted_iota(jnp.int32, f.shape, 1)
    keep = lambda v: jnp.where(lane < heads, v, 0.0)
    hi = f.astype(BF16).astype(F32)
    mid = (f - hi).astype(BF16).astype(F32)
    lo = f - hi - mid
    return (keep(hi) + pltpu.roll(keep(mid), heads, 1) + pltpu.roll(keep(lo), 2 * heads, 1)).astype(BF16)


def expander(width, first_head, head_dim, heads):
    row = lax.broadcasted_iota(jnp.int32, (LANES, width), 0)
    lane = lax.broadcasted_iota(jnp.int32, (LANES, width), 1)
    head = row - jnp.where(row >= 2 * heads, 2 * heads, jnp.where(row >= heads, heads, 0))
    low = (head - first_head) * head_dim
    return jnp.where((lane >= low) & (lane < low + head_dim) & (row < 3 * heads), 1.0, 0.0).astype(BF16)


def silu(a):
    return a * (1.0 / (1.0 + jnp.exp(-a)))


def weight_copies(pieces, offsets_ref, number, weight, sem, rows, low, high):
    copies = []
    for piece in pieces:
        for part in range(piece.shape[0] // rows):
            to = pl.multiple_of(offsets_ref[number], 16)
            at = pl.ds(low, high - low)
            copies.append(
                pltpu.make_async_copy(
                    piece.at[pl.ds(part * rows, rows), at], weight.at[pl.ds(to, rows), at], sem
                )
            )
            number += 1
    return copies


def begin(copies):
    for copy in copies:
        copy.start()


def finish(copies):
    for copy in copies:
        copy.wait()


def project_kernel(count, rows, number, base, extra, has_step, *refs):
    offsets_ref, blocks_ref = refs[:2]
    pieces = refs[2 : 2 + count]
    refs = refs[2 + count :]
    if has_step:
        ext, taps, bias, scalars = refs[:4]
        out, step_out, cum_out, weight, acc, sem = refs[4:]
    else:
        ext, taps, bias = refs[:3]
        out, weight, acc, sem = refs[3:]
    slots = out.shape[0]
    width = weight.shape[1]
    tiles = out.shape[1] // TILE
    plain = tiles - (1 if has_step else 0)
    first_tiles = 1
    cut = first_tiles * TILE
    inputs = weight_copies(pieces, offsets_ref, number, weight, sem.at[0], rows, 0, cut)
    others = weight_copies(pieces, offsets_ref, number, weight, sem.at[1], rows, cut, width)
    begin(inputs)
    begin(others)
    finish(inputs)
    kernel = taps.shape[0]

    def epilogue(t, slot):
        column = jnp.where(t < plain, base + t * TILE, extra)
        from_ = pl.ds(pl.multiple_of(column, LANES), TILE)
        at = pl.ds(pl.multiple_of(t * TILE, TILE), TILE)
        tap = taps[:, from_]
        start = bias[:, from_]
        for block in range(slots // BLOCK):
            total = start + jnp.zeros((BLOCK, TILE), F32)
            for k in range(kernel):
                first = HALO - (kernel - 1) + k + block * BLOCK
                total = total + tap[k : k + 1, :] * acc[slot, first : first + BLOCK, :]
            out[block * BLOCK : (block + 1) * BLOCK, at] = silu(total).astype(BF16)

    def tile(t, carry):
        epilogue(jnp.maximum(t - 1, 0), lax.rem(t + 1, 2))
        at = pl.ds(pl.multiple_of(t * TILE, TILE), TILE)
        acc[lax.rem(t, 2)] = dot(ext[...], weight[:, at]).astype(BF16).astype(F32)
        return carry

    lax.fori_loop(0, first_tiles, tile, 0)
    finish(others)
    lax.fori_loop(first_tiles, tiles, tile, 0)
    if has_step:
        first = tiles * TILE
        raw_all = dot(ext[HALO:, :], weight[:, first : first + LANES]).astype(BF16).astype(F32)
        row = lax.broadcasted_iota(jnp.int32, (BLOCK, BLOCK), 0)
        col = lax.broadcasted_iota(jnp.int32, (BLOCK, BLOCK), 1)
        lower = jnp.where(row >= col, 1.0, 0.0).astype(BF16)
        token = lax.broadcasted_iota(jnp.int32, (BLOCK, LANES), 0)
        for block in range(slots // BLOCK):
            low, high = block * BLOCK, (block + 1) * BLOCK
            a = raw_all[low:high] + scalars[0:1, :]
            size = jnp.maximum(a, 0.0) + jnp.log1p(jnp.exp(-jnp.abs(a)))
            size = jnp.where(token + low < blocks_ref[0] * BLOCK, size, 0.0)
            hi, mid, lo = split3(-(size * scalars[1:2, :]))
            step_out[low:high, :] = size
            cum_out[low:high, :] = dot(lower, hi) + dot(lower, mid) + dot(lower, lo)
    epilogue(tiles - 1, (tiles - 1) % 2)


def summary_kernel(first_head, head_dim, heads, x_ref, bc_ref, cum_ref, step_ref, starts, summary, state, total):
    width = x_ref.shape[1]
    state_width = bc_ref.shape[1] // 2
    block = pl.program_id(0)

    @pl.when(block == 0)
    def _():
        state[...] = jnp.zeros_like(state)
        total[...] = jnp.ones_like(total)

    onehot = expander(width, first_head, head_dim, heads)
    cum = cum_ref[...]
    last = cum[BLOCK - 1 : BLOCK, :]
    to_end = dot(packed(jnp.exp(last - cum) * step_ref[...], heads), onehot)
    hi, lo = split2(x_ref[...].astype(F32) * to_end)
    b = bc_ref[:, :state_width]
    local = dot_rows(b, hi) + dot_rows(b, lo)
    decay = dot(packed(jnp.exp(last) + jnp.zeros((8, LANES), F32), heads), onehot)
    starts[0] = state[...]
    state[...] = decay[:1, :] * state[...] + local
    total[...] = total[...] * decay

    @pl.when(block == pl.num_programs(0) - 1)
    def _():
        quarter = summary.shape[2]
        for q in range(summary.shape[0]):
            summary[q, :state_width, :] = state[:, q * quarter : (q + 1) * quarter]
            summary[q, state_width:, :] = total[:, q * quarter : (q + 1) * quarter]


def inner_kernel(first_head, head_dim, heads, x_ref, bc_ref, cum_ref, step_ref, scalars, starts, y_ref):
    width = x_ref.shape[1]
    state_width = bc_ref.shape[1] // 2
    half = BLOCK // 2
    b = bc_ref[:, :state_width]
    c = bc_ref[:, state_width:]
    scores = lax.dot_general(c, b, (((1,), (1,)), ((), ())), preferred_element_type=F32)
    cum = cum_ref[...]
    step = step_ref[...]
    scaled = cum * LOG2E
    log_step = jnp.where(step > 0.0, jnp.log(step) * LOG2E, -1e30)
    across = (log_step - scaled).T
    onehot = expander(width, first_head, head_dim, heads)
    reach_decay = dot(packed(jnp.exp(cum), heads), onehot)
    skip = dot(packed(scalars[2:3, :] + jnp.zeros((8, LANES), F32), heads), onehot)
    row = lax.broadcasted_iota(jnp.int32, (half, half), 0)
    col = lax.broadcasted_iota(jnp.int32, (half, half), 1)
    causal = row >= col
    lane = lax.broadcasted_iota(jnp.int32, (1, LANES), 1)
    per = LANES // head_dim
    cc = jnp.concatenate([c, c], axis=1)
    for group in range(width // LANES):
        at = slice(group * LANES, (group + 1) * LANES)
        x = x_ref[:, at]
        reach = dot(cc, jnp.concatenate(split2(starts[0, :, at]), axis=0))
        base = reach * reach_decay[:, at] + skip[:1, at] * x.astype(F32)
        top, low = base[:half], base[half:]
        for member in range(per):
            head = first_head + group * per + member
            mine = (lane >= member * head_dim) & (lane < (member + 1) * head_dim)
            own = jnp.where(mine, x, jnp.zeros_like(x))
            down = scaled[:, head : head + 1]
            right = across[head : head + 1, :]
            m00 = jnp.where(causal, jnp.exp2(down[:half] + right[:, :half]) * scores[:half, :half], 0.0)
            m10 = jnp.exp2(down[half:] + right[:, :half]) * scores[half:, :half]
            m11 = jnp.where(causal, jnp.exp2(down[half:] + right[:, half:]) * scores[half:, half:], 0.0)
            hi, lo = split2(m00)
            top = top + (dot(hi, own[:half]) + dot(lo, own[:half]))
            hi, lo = split2(jnp.concatenate([m10, m11], axis=1))
            low = low + (dot(hi, own) + dot(lo, own))
        y_ref[:half, at] = top
        y_ref[half:, at] = low


def gate_kernel(count, rows, number, *refs):
    offsets_ref = refs[0]
    pieces = refs[1 : 1 + count]
    ext, out, weight, sem = refs[1 + count :]
    width = weight.shape[1]
    inputs = weight_copies(pieces, offsets_ref, number, weight, sem.at[0], rows, 0, TILE)
    others = weight_copies(pieces, offsets_ref, number, weight, sem.at[1], rows, TILE, width)
    begin(inputs)
    begin(others)
    finish(inputs)

    def tile(t, carry):
        at = pl.ds(pl.multiple_of(t * TILE, TILE), TILE)
        out[:, at] = dot(ext[HALO:, :], weight[:, at]).astype(BF16)
        return carry

    tile(0, 0)
    finish(others)
    lax.fori_loop(1, width // TILE, tile, 0)


def final_kernel(head_dim, heads, blocks_ref, *refs):
    gates, ys, states = refs[:2], refs[2:4], refs[4:6]
    bc_ref, cum_ref, gain, out, earlier, gated = refs[6:]
    state_width = bc_ref.shape[1] // 2
    whole = out.shape[1]
    block = pl.program_id(0)

    @pl.when(block == 0)
    def _():
        earlier[...] = jnp.zeros_like(earlier)

    def part(pair, column):
        first = pair[0].shape[1]
        ref, low = (pair[0], column) if column < first else (pair[1], column - first)
        return ref[:, low : low + TILE]

    cum = cum_ref[...]
    factors = packed(jnp.exp(cum + earlier[:1, :]), heads)
    earlier[...] = earlier[...] + cum[BLOCK - 1 : BLOCK, :]
    c = bc_ref[:, state_width:]
    twice = jnp.concatenate([c, c], axis=1)
    squares = jnp.zeros((BLOCK, LANES), F32)
    for column in range(0, whole, TILE):
        both = jnp.concatenate(split2(part(states, column)), axis=0)
        reach = dot(twice, both)
        decay = dot(factors, expander(TILE, column // head_dim, head_dim, heads))
        value = (part(ys, column) + decay * reach) * silu(part(gates, column).astype(F32))
        gated[:, column : column + TILE] = value
        square = value * value
        for lane in range(0, TILE, LANES):
            squares = squares + square[:, lane : lane + LANES]
    scale = lax.rsqrt(jnp.sum(squares, axis=1, keepdims=True) / whole + 1e-05)
    live = block < blocks_ref[0]
    for column in range(0, whole, TILE):
        at = slice(column, column + TILE)
        out[:, at] = jnp.where(live, gated[:, at] * scale * gain[:, at], 0.0).astype(BF16)


ANY = pl.BlockSpec(memory_space=pl.ANY)
FULL = pl.BlockSpec(memory_space=pltpu.VMEM)
SCALARS = pl.BlockSpec(memory_space=pltpu.SMEM)
MIB = 1024 * 1024


def like(shape, dtype):
    return jax.ShapeDtypeStruct(shape, dtype)


def call(kernel, in_specs, out_shape, scratch, flops, limit, *args):
    return pl.pallas_call(
        kernel,
        in_specs=in_specs,
        out_specs=jax.tree.map(lambda _: FULL, out_shape),
        out_shape=out_shape,
        scratch_shapes=scratch,
        cost_estimate=pl.CostEstimate(flops=flops, bytes_accessed=16_000_000, transcendentals=0),
        compiler_params=pltpu.CompilerParams(vmem_limit_bytes=limit * MIB),
    )(*args)


def project(pieces, rows, number, offsets, blocks, ext, taps, bias, base, extra, scalars):
    slots, depth = ext.shape[0] - HALO, ext.shape[1]
    width = pieces[0].shape[1]
    has_step = scalars is not None
    conv = width - LANES if has_step else width
    out = [like((slots, conv), BF16)]
    if has_step:
        out += [like((slots, LANES), F32)] * 2
    return call(
        functools.partial(project_kernel, len(pieces), rows, number, base, extra, has_step),
        [SCALARS] * 2 + [ANY] * len(pieces) + [FULL] * (4 if has_step else 3),
        out,
        [
            VMEM((depth, width), BF16),
            VMEM((2, slots + HALO, TILE), F32),
            pltpu.SemaphoreType.DMA((2,)),
        ],
        2 * slots * depth * width, 18,
        offsets, blocks, *pieces, ext, taps, bias, *([scalars] if has_step else []),
    )


def by_block(width, column=0):
    return pl.BlockSpec((BLOCK, width), lambda i: (i, column))


def summarize(x, width, first, bc_at, state_width, cum, step, first_head, head_dim, heads, parts):
    slots = x.shape[0]
    count = slots // BLOCK
    shape = (parts, state_width + 8, width // parts)
    return pl.pallas_call(
        functools.partial(summary_kernel, first_head, head_dim, heads),
        name="summary",
        grid=(count,),
        in_specs=[by_block(width), by_block(2 * state_width, bc_at), by_block(LANES), by_block(LANES)],
        out_specs=[
            pl.BlockSpec((1, state_width, width), lambda i: (i, 0, 0)),
            pl.BlockSpec(shape, lambda i: (0, 0, 0)),
        ],
        out_shape=[like((count, state_width, width), F32), like(shape, F32)],
        scratch_shapes=[VMEM((state_width, width), F32), VMEM((8, width), F32)],
        cost_estimate=pl.CostEstimate(flops=4 * slots * state_width * width, bytes_accessed=8_000_000, transcendentals=0),
        compiler_params=pltpu.CompilerParams(vmem_limit_bytes=14 * MIB),
    )(x, first, cum, step)


def inner(x, width, first, bc_at, state_width, cum, step, scalars, starts, first_head, head_dim, heads):
    slots = x.shape[0]
    return pl.pallas_call(
        functools.partial(inner_kernel, first_head, head_dim, heads),
        name="inner",
        grid=(slots // BLOCK,),
        in_specs=[
            by_block(width), by_block(2 * state_width, bc_at), by_block(LANES), by_block(LANES),
            pl.BlockSpec((8, LANES), lambda i: (0, 0)),
            pl.BlockSpec((1, state_width, width), lambda i: (i, 0, 0)),
        ],
        out_specs=by_block(width),
        out_shape=like((slots, width), F32),
        cost_estimate=pl.CostEstimate(flops=6 * slots * BLOCK * width, bytes_accessed=8_000_000, transcendentals=0),
        compiler_params=pltpu.CompilerParams(vmem_limit_bytes=15 * MIB),
    )(x, first, cum, step, scalars, starts)


def gate_columns(pieces, rows, number, offsets, ext):
    slots, depth = ext.shape[0] - HALO, ext.shape[1]
    width = pieces[0].shape[1]
    return call(
        functools.partial(gate_kernel, len(pieces), rows, number),
        [SCALARS] + [ANY] * len(pieces) + [FULL],
        like((slots, width), BF16),
        [VMEM((depth, width), BF16), pltpu.SemaphoreType.DMA((2,))],
        2 * slots * depth * width, 15,
        offsets, *pieces, ext,
    )


def finished(blocks, gates, ys, states, first, bc_at, state_width, cum, gain, head_dim, heads):
    slots = cum.shape[0]
    whole = gain.shape[1]
    full = lambda a: pl.BlockSpec(a.shape, lambda i: (0, 0))
    return pl.pallas_call(
        functools.partial(final_kernel, head_dim, heads),
        name="final",
        grid=(slots // BLOCK,),
        in_specs=[SCALARS] + [by_block(a.shape[1]) for a in gates + ys] + [full(a) for a in states]
        + [by_block(2 * state_width, bc_at), by_block(LANES), full(gain)],
        out_specs=by_block(whole),
        out_shape=like((slots, whole), BF16),
        scratch_shapes=[VMEM((8, LANES), F32), VMEM((BLOCK, whole), F32)],
        cost_estimate=pl.CostEstimate(flops=8 * slots * state_width * whole, bytes_accessed=16_000_000, transcendentals=0),
        compiler_params=pltpu.CompilerParams(vmem_limit_bytes=22 * MIB),
    )(blocks, *gates, *ys, *states, first, cum, gain)


PLANE = 4


def routes(planes, cores):
    ids = lambda z, m, c: (z * PLANE + m) * cores + c
    places = [(z, m, c) for z in range(planes) for m in range(PLANE) for c in range(cores)]
    beside = lambda turn: [(ids(z, m, c), ids(z, m ^ (1 if c % 2 == turn else 2), c)) for z, m, c in places]
    return dict(
        long=[[(ids(z, m, c), ids((z + k) % planes, m, c)) for z, m, c in places] for k in range(planes)],
        beside=[beside(0), beside(1)],
        swap=[(ids(z, m, c), ids(z, m, cores - 1 - c)) for z, m, c in places],
        cross=[[(ids(z, m, c), ids(z, m ^ a, c)) for z, m, c in places] for a in range(PLANE)],
        later=[[(ids(z, m, c), ids(z + k, m, c)) for z, m, c in places if z + k < planes] for k in range(planes)],
        after=[(s, s + cores) for s in range((planes * PLANE - 1) * cores)],
    )


def send(value, pairs):
    return lax.ppermute(value, AXES, pairs)


def joined(parts):
    return jnp.concatenate(parts, axis=0)


def along(held, paths, planes):
    return [held] + [send(held, paths["long"][k]) for k in range(1, planes)]


def around(held, paths):
    near = send(held, paths["beside"][0])
    side = send(held, paths["beside"][1])
    return [held, near, side, send(near, paths["beside"][1])]


def offsets_of(paths, planes, cores, rows, long_first):
    if rows % HALO or planes > PLANE:
        return np.zeros((planes * PLANE * cores, 1), np.int32)
    blocks = np.arange(planes * PLANE * cores)[:, None]

    def landed(held, pairs):
        out = np.zeros_like(held)
        for source, target in pairs:
            out[target] = held[source]
        return out

    along = lambda held: [held] + [landed(held, paths["long"][k]) for k in range(1, planes)]

    def around(held):
        near = landed(held, paths["beside"][0])
        return [held, near, landed(held, paths["beside"][1]), landed(near, paths["beside"][1])]

    first, second = (along, around) if long_first else (around, along)
    line = second(np.concatenate(first(blocks), axis=1))
    line = line + [landed(held, paths["swap"]) for held in line]
    return np.concatenate(line, axis=1) * rows


def collect(chunk, paths, planes, cores, rows, long_first):
    if rows % HALO or planes > PLANE:
        count = planes * PLANE * cores
        return [lax.all_gather(chunk, AXES, axis=0, tiled=True)], rows * count
    if long_first:
        line = around(joined(along(chunk, paths, planes)), paths)
    else:
        line = along(joined(around(chunk, paths)), paths, planes)
    return line + [send(held, paths["swap"]) for held in line], rows


def compose(earlier, later, wide):
    decay = later[wide:]
    return jnp.concatenate([decay[:1] * earlier[:wide] + later[:wide], earlier[wide:] * decay], axis=0)


def pick(parts, index):
    rest = (np.uint32(0),) * (parts.ndim - 1)
    return lax.dynamic_slice(parts, (index,) + rest, (1,) + parts.shape[1:])[0]


def carried_in(summary, paths, planes, mine, wide):
    parts = jnp.stack(
        [pick(summary, mine[0])]
        + [send(pick(summary, mine[a]), paths["cross"][a]) for a in range(1, PLANE)]
    )
    members = [pick(parts, mine[m]) for m in range(PLANE)]
    totals = [members[0]]
    for member in members[1:]:
        totals.append(compose(totals[-1], member, wide))
    state = jnp.zeros_like(summary[0, :wide])
    for k in range(planes - 1, 0, -1):
        part = send(totals[-1], paths["later"][k])
        state = part[wide : wide + 1] * state + part[:wide]
    states = jnp.stack([state] + [t[wide : wide + 1] * state + t[:wide] for t in totals[:-1]])
    back = jnp.stack(
        [pick(states, mine[0])]
        + [send(pick(states, mine[a]), paths["cross"][a]) for a in range(1, PLANE)]
    )
    return jnp.concatenate([pick(back, mine[q]) for q in range(PLANE)], axis=1)


def local(tokens, bounds, in_weight, conv_weight, conv_bias, dt_bias, decay_rate, skip_gain, norm_gain):
    cores = lax.axis_size("fsdp")
    planes = lax.axis_size("seq") // PLANE
    paths = routes(planes, cores)
    own = tokens[0]
    rows = in_weight.shape[0]
    tables = [offsets_of(paths, planes, cores, rows, i < LONG_FIRST) for i in range(4)]
    numbers = [sum(t.shape[1] for t in tables[:i]) for i in range(4)]
    table = jnp.asarray(np.concatenate(tables, axis=1), jnp.int32)
    place = (lax.axis_index("seq") * cores + lax.axis_index("fsdp")).astype(jnp.uint32)
    offsets = pick(table, place)
    mine = [(lax.axis_index("seq").astype(jnp.uint32) % PLANE) ^ jnp.uint32(a) for a in range(PLANE)]
    live = bounds[0, 0, 1] - bounds[0, 0, 0]
    in_weight, offsets, mine, live = lax.optimization_barrier((in_weight, offsets, mine, live))
    inner_width = norm_gain.shape[0]
    state_width = (conv_bias.shape[0] - inner_width) // 2
    heads = decay_rate.shape[0]
    head_dim = inner_width // heads
    early = heads // 5 // 8 * 8
    cut = early * head_dim
    gate_cut = inner_width * GATE_SHARE // 10 // TILE * TILE
    blocks = live[None]
    scalars = jnp.pad(jnp.stack([dt_bias, decay_rate, skip_gain]), ((0, 5), (0, LANES - heads)))

    rest = jnp.pad(in_weight[:, 2 * inner_width :], ((0, 0), (0, LANES - heads)))
    chunks = [
        jnp.concatenate([in_weight[:, inner_width : inner_width + cut], rest], axis=1),
        None,
        None,
        in_weight[:, gate_cut:inner_width],
    ]
    chunks[1] = in_weight[:, inner_width + cut : 2 * inner_width]
    chunks[2] = in_weight[:, :gate_cut]
    edge = lax.dynamic_slice_in_dim(own, live * BLOCK - HALO, HALO, 0)
    halo = send(edge, paths["after"])
    ext = jnp.concatenate([halo, own], axis=0)
    weights = [collect(chunk, paths, planes, cores, rows, i < LONG_FIRST) for i, chunk in enumerate(chunks)]

    bias = conv_bias[None]
    first, step, cum = project(
        weights[0][0], weights[0][1], numbers[0], offsets, blocks, ext, conv_weight, bias, 0, inner_width, scalars
    )
    (second,) = project(
        weights[1][0], weights[1][1], numbers[1], offsets, blocks, ext, conv_weight, bias, cut, cut, None
    )
    x = [first, second]
    widths = [cut, inner_width - cut]
    firsts = [0, early]
    bc_at = cut // (2 * state_width)
    parts, states, ys = [], [], []
    for i in range(2):
        parts.append(
            summarize(x[i], widths[i], first, bc_at, state_width, cum, step, firsts[i], head_dim, heads, PLANE)
        )
    for i in range(2):
        states.append(carried_in(parts[i][1], paths, planes, mine, state_width))
    for i in range(2):
        ys.append(
            inner(x[i], widths[i], first, bc_at, state_width, cum, step, scalars, parts[i][0], firsts[i], head_dim, heads)
        )
    gates = []
    for i in range(2):
        gates.append(gate_columns(weights[2 + i][0], weights[2 + i][1], numbers[2 + i], offsets, ext))
    out = finished(blocks, gates, ys, states, first, bc_at, state_width, cum, norm_gain[None], head_dim, heads)
    return out[None]


LONG_FIRST = 3
GATE_SHARE = 8


def solution(mesh):
    whole = P("fsdp", "seq", None)
    in_specs = (whole, whole, P(("seq", "fsdp"), None)) + (P(),) * 6

    return jax.shard_map(local, mesh=mesh, in_specs=in_specs, out_specs=whole, check_vma=False)
```
